128 devices in a mesh: dp: 8 (over y, x_lo), tensor: 16 (over x_hi, z, core).
Axes of the slice: x: 4 (x_hi: 2, x_lo: 2; x = x_hi * 2 + x_lo), y: 4, z: 4, core: 2. Of those that a mesh axis runs over, the one named last changes fastest.
Arguments:
- grad_out: bfloat16 [8192, 8192], P(('dp', 'tensor')), may hold values from -24 to 24
- out_weight: bfloat16 [8192, 8192], P('dp', 'tensor'), may hold values from -0.0625 to 0.0625
- query: bfloat16 [8192, 8192], P('dp', 'tensor'), may hold values from -6 to 6, as said below
- keys: bfloat16 [8192, 512], P('dp'), may hold values from -6 to 6
- values: bfloat16 [8192, 512], P('dp'), may hold values from -6 to 6
- attended: bfloat16 [8192, 8192], P('dp', 'tensor'), may hold values from -6 to 6, as said below
- stats: float32 [64, 8192], P('tensor', 'dp'), as said below
Outputs:
- query_grad: bfloat16 [8192, 8192], P('dp', 'tensor')
- key_grad: bfloat16 [8192, 512], P('dp', 'tensor')
- value_grad: bfloat16 [8192, 512], P('dp', 'tensor')
- weight_grad: bfloat16 [8192, 8192], P('dp', 'tensor')
The draws below stay inside these ranges and needn't reach their ends.
Inputs may be any that keep to these rules, and one draw needn't show every extreme that they name: query, keys and values are independent draws. attended is the causal attention output of the given query, keys and values within each sequence of 1024 rows: query head h uses key head h // 16, scores scaled by 128 ** -0.5, softmax over keys at or before the query. stats[h, t] is the logarithm of the sum of exp(score) over the keys that row t of head h attends to, for the same scores.
All inputs are finite; a program needn't handle non-finite values.
Results may differ from the reference program's by a relative error of at most 0.013.
Values may be sent and summed in bfloat16 or wider, within the bound.
No kernel may reach another device: no remote copies, remote signals or barrier semaphores. Data moves between devices by JAX's collectives and lax.ppermute only.
A program may use at most 192 MiB of HBM per device.

```python
import jax
import jax.numpy as jnp
from jax import lax

D = 8192
HD = 128
GROUP = 16
LEN = 1024
HEADS = 64
KV_HEADS = 4
TOKENS = 8192


def draw_inputs(key):
    key_query = jax.random.fold_in(key, 101)
    key_keys = jax.random.fold_in(key, 202)
    key_values = jax.random.fold_in(key, 303)
    query = jnp.clip(jax.random.normal(key_query, (TOKENS, HEADS * HD), jnp.float32), -6.0, 6.0)
    keys = jnp.clip(jax.random.normal(key_keys, (TOKENS, KV_HEADS * HD), jnp.float32), -6.0, 6.0)
    values = jnp.clip(jax.random.normal(key_values, (TOKENS, KV_HEADS * HD), jnp.float32), -6.0, 6.0)
    return (query.astype(jnp.bfloat16), keys.astype(jnp.bfloat16), values.astype(jnp.bfloat16))


def forward_pass(key):
    query, keys, values = draw_inputs(key)
    seq_count = TOKENS // LEN
    query_split = query.astype(jnp.float32).reshape(seq_count, LEN, KV_HEADS, GROUP, HD)
    query_split = query_split.transpose(0, 2, 3, 1, 4).reshape(seq_count * KV_HEADS, GROUP, LEN, HD)
    keys_split = keys.astype(jnp.float32).reshape(seq_count, LEN, KV_HEADS, HD)
    keys_split = keys_split.transpose(0, 2, 1, 3).reshape(seq_count * KV_HEADS, LEN, HD)
    values_split = values.astype(jnp.float32).reshape(seq_count, LEN, KV_HEADS, HD)
    values_split = values_split.transpose(0, 2, 1, 3).reshape(seq_count * KV_HEADS, LEN, HD)
    positions = jnp.arange(LEN, dtype=jnp.int32)
    causal = positions[:, None] >= positions[None, :]

    def single(inputs):
        query_group, key_one, value_one = inputs
        scores = jnp.einsum('gqd,kd->gqk', query_group, key_one) * HD ** (-0.5)
        masked = jnp.where(causal[None], scores, -1e+30)
        highest = jnp.max(masked, axis=2, keepdims=True)
        log_total = highest[:, :, 0] + jnp.log(jnp.sum(jnp.exp(masked - highest), axis=2))
        weights_soft = jnp.exp(masked - log_total[:, :, None])
        output = jnp.einsum('gqk,kd->gqd', weights_soft, value_one)
        return (output, log_total)
    outputs, log_totals = lax.map(single, (query_split, keys_split, values_split))
    attended = outputs.reshape(seq_count, KV_HEADS, GROUP, LEN, HD).transpose(0, 3, 1, 2, 4)
    attended = attended.reshape(TOKENS, HEADS * HD)
    stats = log_totals.reshape(seq_count, KV_HEADS, GROUP, LEN).transpose(1, 2, 0, 3).reshape(HEADS, TOKENS)
    return (attended, stats)


def draw_query(key, part):
    return draw_inputs(key)[0]


def draw_keys(key, part):
    return draw_inputs(key)[1]


def draw_values(key, part):
    return draw_inputs(key)[2]


def draw_attended(key, part):
    return forward_pass(key)[0].astype(jnp.bfloat16)


def draw_stats(key, part):
    return forward_pass(key)[1].astype(jnp.float32)


def spiked(drawn, rng, source, target, shards_of, factor):
    owner, partner = [(jnp.arange(drawn.shape[dim]) // (drawn.shape[dim] // shards_of)).reshape([-1 if axis == dim else 1 for axis in range(drawn.ndim)]) for dim in (source, target)]
    chosen = jax.random.permutation(rng, shards_of)[partner]
    strong = (owner == chosen) | (owner == (partner + shards_of // 2) % shards_of)
    return jnp.where(strong, factor * drawn, drawn)


def block_levels(rng, dims, split, low, high):
    factor_of = 1.0
    for dim, blocks in split:
        heights = jax.random.uniform(jax.random.fold_in(jax.random.fold_in(rng, 6), dim), (blocks,), jnp.float32, low / len(split), high / len(split))
        factor_of = factor_of * jnp.repeat(jnp.exp(heights), dims[dim] // blocks).reshape((-1,) + (1,) * (len(dims) - 1 - dim))
    return factor_of


def noise(rng, dims, width, reach, cuts=(), kind=jnp.bfloat16):
    loudness = block_levels(rng, dims, cuts, -0.22, 0.18) if cuts else 1.0
    entries = jax.random.normal(rng, dims, jnp.float32) * width * loudness
    return jnp.minimum(jnp.maximum(entries, -reach), reach).astype(kind)


def gaussian_with(own_key, extent, deviation, reach, cuts, heavy, kind=jnp.bfloat16):
    entries = deviation * jax.random.normal(own_key, extent, jnp.float32)
    if cuts:
        entries = entries * block_levels(own_key, extent, cuts, -0.22, 0.18)
    return jnp.clip(spiked(entries, jax.random.fold_in(own_key, 3), *heavy), -reach, reach).astype(kind)


def setup_inputs(seed: int = 0) -> dict:
    key_of = jax.random.split(jax.random.key(seed), 8)
    return {
        "grad_out": gaussian_with(key_of[0], (TOKENS, D), 1.0, 24.0, ((0, 128),), (0, 1, 128, 5.5)),
        "out_weight": noise(key_of[1], (D, HEADS * HD), D ** -0.5, 0.0625, ((0, 8), (1, 16))),
        "query": draw_query(jax.random.fold_in(key_of[7], 71), 0),
        "keys": draw_keys(jax.random.fold_in(key_of[7], 71), 0),
        "values": draw_values(jax.random.fold_in(key_of[7], 71), 0),
        "attended": draw_attended(jax.random.fold_in(key_of[7], 71), 0),
        "stats": draw_stats(jax.random.fold_in(key_of[7], 71), 0),
    }


def split_heads(array, seq_count):
    shaped = array.reshape(seq_count, LEN, KV_HEADS, GROUP, HD).transpose(0, 2, 3, 1, 4)
    return shaped.reshape(seq_count * KV_HEADS, GROUP, LEN, HD)

def join_heads(array, seq_count):
    shaped = array.reshape(seq_count, KV_HEADS, GROUP, LEN, HD).transpose(0, 3, 1, 2, 4)
    return shaped.reshape(seq_count * LEN, KV_HEADS * GROUP * HD)

def split_keys(array, seq_count):
    shaped = array.reshape(seq_count, LEN, KV_HEADS, HD).transpose(0, 2, 1, 3)
    return shaped.reshape(seq_count * KV_HEADS, LEN, HD)

def join_keys(array, seq_count):
    shaped = array.reshape(seq_count, KV_HEADS, LEN, HD).transpose(0, 2, 1, 3)
    return shaped.reshape(seq_count * LEN, KV_HEADS * HD)

def head_grads(inputs):
    query_group, key_one, value_one, attended_group, grad_group, stats_group = inputs
    score_scale = HD ** (-0.5)
    query_wide = query_group.astype(jnp.float32)
    key_wide = key_one.astype(jnp.float32)
    grad_wide = grad_group.astype(jnp.float32)
    positions = jnp.arange(LEN, dtype=jnp.int32)
    causal = positions[:, None] >= positions[None, :]
    scores = jnp.einsum('gqd,kd->gqk', query_wide, key_wide) * score_scale
    attention = jnp.where(causal[None], jnp.exp(scores - stats_group[:, :, None]), 0.0)
    attention_low = lax.optimization_barrier(attention.astype(jnp.bfloat16)).astype(jnp.float32)
    grad_attention = jnp.einsum('gqd,kd->gqk', grad_wide, value_one.astype(jnp.float32))
    row_offset = lax.optimization_barrier(jnp.sum(grad_wide * attended_group.astype(jnp.float32), axis=2))
    grad_scores = attention * (grad_attention - row_offset[:, :, None])
    grad_scores = lax.optimization_barrier(grad_scores.astype(jnp.bfloat16)).astype(jnp.float32)
    query_grad = (jnp.einsum('gqk,kd->gqd', grad_scores, key_wide) * score_scale).astype(jnp.bfloat16)
    key_grad = (jnp.einsum('gqk,gqd->kd', grad_scores, query_wide) * score_scale).astype(jnp.bfloat16)
    value_grad = jnp.einsum('gqk,gqd->kd', attention_low, grad_wide).astype(jnp.bfloat16)
    return (query_grad, key_grad, value_grad)

def reference(grad_out, out_weight, query, keys, values, attended, stats):
    seq_count = TOKENS // LEN
    grad_att = jnp.dot(grad_out, out_weight, preferred_element_type=jnp.float32).astype(jnp.bfloat16)
    grad_seqs = grad_out.reshape(seq_count, LEN, D)
    attended_seqs = attended.reshape(seq_count, LEN, HEADS * HD)

    def add_grad(running, pair):
        grad_block, attended_block = pair
        grad_term = lax.dot_general(grad_block, attended_block, (((0,), (0,)), ((), ())), preferred_element_type=jnp.float32)
        rounded = lax.optimization_barrier(grad_term.astype(jnp.bfloat16))
        return (running + rounded.astype(jnp.float32), None)
    weight_sum, _ = lax.scan(add_grad, jnp.zeros((D, HEADS * HD), jnp.float32), (grad_seqs, attended_seqs))
    weight_grad = weight_sum.astype(jnp.bfloat16)
    stats_split = stats.reshape(KV_HEADS, GROUP, seq_count, LEN).transpose(2, 0, 1, 3)
    stats_split = stats_split.reshape(seq_count * KV_HEADS, GROUP, LEN)
    query_parts, key_parts, value_parts = lax.map(head_grads, (split_heads(query, seq_count), split_keys(keys, seq_count), split_keys(values, seq_count), split_heads(attended, seq_count), split_heads(grad_att, seq_count), stats_split))
    query_grad = join_heads(query_parts, seq_count)
    key_grad = join_keys(key_parts, seq_count)
    value_grad = join_keys(value_parts, seq_count)
    return (query_grad, key_grad, value_grad, weight_grad)
```

```python
import functools

import jax
import jax.numpy as jnp
import numpy as np
from jax import lax
from jax.experimental import pallas as pl
from jax.experimental.pallas import tpu as pltpu
from jax.sharding import Mesh
from jax.sharding import PartitionSpec as P

HD = 128
HEAD_DEV = 4
GROUP = 16
SCALE = HD ** (-0.5)
DP = ("y", "xl")
TENSOR = ("xh", "z", "c")
PIECE = 64
BLOCK = 1024
TOKENS_SEQ = 1024


def swap(x, axis):
    return lax.ppermute(x, axis, [(0, 1), (1, 0)])


def along(x, axis):
    n = lax.axis_size(axis)
    pairs = []
    for i in range(n):
        pairs.append((2 * i, 2 * ((i + 1) % n)))
        pairs.append((2 * i + 1, 2 * ((i - 1) % n) + 1))
    return lax.ppermute(x, (axis, "c"), pairs)


def gather_weight(own):
    def near_blocks(mine):
        other = swap(mine, "c")
        near = along(mine, "y")
        near_other = along(other, "y")
        return [mine, near, swap(near_other, "c")]

    blocks = near_blocks(own)
    far = along(blocks[1], "y")
    partner = swap(own, "xl")
    far_partner = swap(far, "xl")
    return blocks + [far] + near_blocks(partner) + [far_partner]


def weight_order(y, xl, step):
    moved = np.array([0, -1, 1, 2] * 2, np.int32)
    flipped = np.repeat(np.array([0, 1], np.int32), 4)
    return (y + step * moved + 4) % 4 * 2 + (xl + flipped) % 2


def gather_rows(own):
    def ring(mine):
        other = swap(mine, "c")
        near = along(mine, "z")
        near_other = along(other, "z")
        far = along(near, "z")
        return [
            mine,
            other,
            near,
            near_other,
            swap(near, "c"),
            swap(near_other, "c"),
            far,
            swap(far, "c"),
        ]

    partner = swap(own, "xh")
    return ring(own) + ring(partner)


def row_order(xh, z, c, step):
    moved = np.array([0, 0, -1, -1, 1, 1, 2, 2] * 2, np.int32)
    core = np.array([0, 1, 0, 1, 1, 0, 0, 1] * 2, np.int32)
    flipped = np.repeat(np.array([0, 1], np.int32), 8)
    return (xh + flipped) % 2 * 8 + (z + step * moved + 4) % 4 * 2 + (c + core) % 2


def load_rows(pieces, rows):
    for at, piece in enumerate(pieces):
        rows[at * PIECE : (at + 1) * PIECE, :] = piece[...]


def terms_kernel(order, dest, side, *refs, count):
    pieces = refs[:16]
    attended = refs[16:18]
    outs = refs[18 : 18 + count]
    rows, right = refs[18 + count :]
    step = pl.program_id(0)

    @pl.when(step == 0)
    def _():
        for at in range(16):
            start = pl.multiple_of(order[at] * PIECE, PIECE)
            for which in range(2):
                right[which, at * PIECE : (at + 1) * PIECE, :] = attended[which][
                    pl.ds(start, PIECE), :
                ]

    load_rows(pieces, rows)
    total = lax.dot_general(
        rows[...], right[side[step]], (((0,), (0,)), ((), ())), preferred_element_type=jnp.float32
    ).astype(jnp.bfloat16)
    for at in range(count):

        @pl.when(step == at)
        def _():
            outs[at][...] = total


def terms(order, dest, side, pieces, attended, attended_other):
    count = dest.shape[0]
    cols = attended.shape[1]
    whole = pl.BlockSpec((BLOCK, cols), lambda i, order, dest, side: (0, 0))
    piece = pl.BlockSpec((PIECE, BLOCK), lambda i, order, dest, side: (0, dest[i]))
    return pl.pallas_call(
        functools.partial(terms_kernel, count=count),
        grid_spec=pltpu.PrefetchScalarGridSpec(
            num_scalar_prefetch=3,
            grid=(count,),
            in_specs=[piece] * 16 + [whole] * 2,
            out_specs=[whole] * count,
            scratch_shapes=[
                pltpu.VMEM((TOKENS_SEQ, BLOCK), jnp.bfloat16),
                pltpu.VMEM((2, TOKENS_SEQ, cols), jnp.bfloat16),
            ],
        ),
        out_shape=[jax.ShapeDtypeStruct((BLOCK, cols), jnp.bfloat16)] * count,
        cost_estimate=pl.CostEstimate(
            flops=2 * count * BLOCK * cols * TOKENS_SEQ,
            bytes_accessed=count * 3 * 2**20,
            transcendentals=0,
        ),
    )(order, dest, side, *pieces, attended, attended_other)


def dot_kernel(order, place, *refs):
    pieces = refs[:16]
    weights = refs[16:24]
    out, rows, total = refs[24:]
    at_block = pl.program_id(0)
    load_rows(pieces, rows)

    for at in range(8):

        @pl.when(at_block == at)
        def _():
            product = jnp.dot(rows[...], weights[at][...], preferred_element_type=jnp.float32)
            if at == 0:
                total[...] = product
            else:
                total[...] += product

    @pl.when(at_block == 7)
    def _():
        for at in range(16):
            start = pl.multiple_of(order[at] * PIECE, PIECE)
            out[pl.ds(start, PIECE), :] = total[at * PIECE : (at + 1) * PIECE, :].astype(
                jnp.bfloat16
            )


def grad_attention_rows(order, place, pieces, weights):
    cols = weights[0].shape[1]
    return pl.pallas_call(
        dot_kernel,
        grid_spec=pltpu.PrefetchScalarGridSpec(
            num_scalar_prefetch=2,
            grid=(8,),
            in_specs=[pl.BlockSpec((PIECE, BLOCK), lambda i, order, place: (0, place[i]))] * 16
            + [pl.BlockSpec((BLOCK, cols), lambda i, order, place: (0, 0))] * 8,
            out_specs=pl.BlockSpec((TOKENS_SEQ, cols), lambda i, order, place: (0, 0)),
            scratch_shapes=[
                pltpu.VMEM((TOKENS_SEQ, BLOCK), jnp.bfloat16),
                pltpu.VMEM((TOKENS_SEQ, cols), jnp.float32),
            ],
        ),
        out_shape=jax.ShapeDtypeStruct((TOKENS_SEQ, cols), jnp.bfloat16),
        cost_estimate=pl.CostEstimate(
            flops=2 * TOKENS_SEQ * cols * 8 * BLOCK, bytes_accessed=24 * 2**20, transcendentals=0
        ),
    )(order, place, *pieces, *weights)


QB = 256


def head_kernel(query, key, value, grad, attended, stats, query_grad, key_part, value_part):
    head = pl.program_id(0)

    @pl.when(head == 0)
    def _():
        key_part[...] = jnp.zeros_like(key_part)
        value_part[...] = jnp.zeros_like(value_part)

    for block in range(TOKENS_SEQ // QB):
        at = slice(block * QB, (block + 1) * QB)
        seen = (block + 1) * QB
        q = query[at, :]
        g = grad[at, :]
        k = key[:seen, :]
        v = value[:seen, :]
        contract = (((1,), (1,)), ((), ()))
        scores = lax.dot_general(k, q, contract, preferred_element_type=jnp.float32) * SCALE
        attention = jnp.exp(scores - stats[pl.ds(head, 1), at])
        rows = lax.broadcasted_iota(jnp.int32, (seen, QB), 0)
        cols = lax.broadcasted_iota(jnp.int32, (seen, QB), 1) + block * QB
        attention = jnp.where(rows <= cols, attention, 0.0)
        grad_attention = lax.dot_general(v, g, contract, preferred_element_type=jnp.float32)
        offset = g.astype(jnp.float32) * attended[at, :].astype(jnp.float32)
        offset = jnp.sum(offset.T, axis=0, keepdims=True)
        grad_scores = attention * (grad_attention - offset)
        grad_scores = grad_scores.astype(jnp.bfloat16)
        low = attention.astype(jnp.bfloat16)
        value_part[:seen, :] += jnp.dot(low, g, preferred_element_type=jnp.float32)
        key_part[:seen, :] += SCALE * jnp.dot(grad_scores, q, preferred_element_type=jnp.float32)
        back = lax.dot_general(
            grad_scores, k, (((0,), (0,)), ((), ())), preferred_element_type=jnp.float32
        )
        query_grad[at, :] = (back * SCALE).astype(jnp.bfloat16)


def attention_grads(head_at, query, keys, values, grad_att, attended, stats):
    length = query.shape[0]
    column = pl.BlockSpec((length, HD), lambda h, at: (0, h))
    shared = pl.BlockSpec((length, HD), lambda h, at: (0, at[0]))
    row = pl.BlockSpec((HEAD_DEV, length), lambda h, at: (0, 0))
    total = pl.BlockSpec((length, HD), lambda h, at: (0, 0))

    def kernel(at, *refs):
        head_kernel(*refs)

    return pl.pallas_call(
        kernel,
        grid_spec=pltpu.PrefetchScalarGridSpec(
            num_scalar_prefetch=1,
            grid=(HEAD_DEV,),
            in_specs=[column, shared, shared, column, column, row],
            out_specs=[column, total, total],
        ),
        out_shape=[
            jax.ShapeDtypeStruct(query.shape, jnp.bfloat16),
            jax.ShapeDtypeStruct((length, HD), jnp.float32),
            jax.ShapeDtypeStruct((length, HD), jnp.float32),
        ],
        cost_estimate=pl.CostEstimate(
            flops=10 * HEAD_DEV * length * length * HD,
            bytes_accessed=6 * 2**20,
            transcendentals=HEAD_DEV * length * length,
        ),
    )(head_at, query, keys, values, grad_att, attended, stats)


def halved(parts, axis, pairs, upper):
    half = parts.shape[2] // 2
    lower_cols = parts[:, :, :half]
    upper_cols = parts[:, :, half:]
    kept = jnp.where(upper, upper_cols, lower_cols)
    sent = jnp.where(upper, lower_cols, upper_cols)
    got = lax.ppermute(sent.astype(jnp.bfloat16), axis, pairs)
    return kept + got.astype(jnp.float32)


def added(*parts):
    total = parts[0].astype(jnp.float32)
    for part in parts[1:]:
        total = total + part.astype(jnp.float32)
    return total.astype(jnp.bfloat16)


def weight_sums(order, pieces, attended, y, xl, step):
    attended_other = swap(attended, "c")

    def dests(moved, core, flipped):
        moved = np.array(moved, np.int32) + step * np.array(core, np.int32) + 4
        return (y + moved) % 4 * 2 + (xl + np.array(flipped, np.int32)) % 2

    def call(dest, side):
        side = jnp.array(side, jnp.int32)
        return terms(order, dest, side, pieces, attended, attended_other)

    far_p, other_p, near_p, other_o = call(
        dests([2, 0, 0, 0], [0, 1, 1, 1], [1, 1, 1, 0]), [0, 1, 0, 1]
    )
    far_o, near_o, own_p, own_o = call(
        dests([2, 0, 0, 0], [0, 1, 0, 0], [0, 0, 1, 0]), [0, 0, 0, 0]
    )
    far = added(far_o, swap(far_p, "xl"))
    far = along(far, "y")
    near_p = along(near_p, "y")
    near_o = along(added(near_o, far), "y")
    other_p = swap(along(other_p, "y"), "c")
    other_o = swap(along(other_o, "y"), "c")
    partner = swap(added(own_p, near_p, other_p), "xl")
    return added(own_o, other_o, partner, near_o)


def per_device(grad_out, out_weight, query, keys, values, attended, stats):
    y, xl, xh, z, c = (lax.axis_index(name) for name in ("y", "xl", "xh", "z", "c"))
    step = 1 - 2 * c
    pieces = gather_rows(grad_out)
    weights = gather_weight(out_weight)
    order = row_order(xh, z, c, step)
    weight_grad = weight_sums(order, pieces, attended, y, xl, step)
    grad_att = grad_attention_rows(order, weight_order(y, xl, step), pieces, weights)
    key_head = (xh * 8 + z * 2 + c) * HEAD_DEV // GROUP
    query_grad, key_part, value_part = attention_grads(
        key_head.reshape(1), query, keys, values, grad_att, attended, stats
    )
    parts = jnp.stack([key_part, value_part])
    parts = halved(parts, "z", [(0, 1), (1, 0), (2, 3), (3, 2)], z % 2 == 1)
    parts = halved(parts, "c", [(0, 1), (1, 0)], c == 1)
    key_grad = parts[0].astype(jnp.bfloat16)
    value_grad = parts[1].astype(jnp.bfloat16)
    return (query_grad, key_grad, value_grad, weight_grad)


def solution(mesh):
    torus = Mesh(mesh.devices.reshape(4, 2, 2, 4, 2), DP + TENSOR)
    in_specs = (
        P(DP + TENSOR, None),
        P(DP, TENSOR),
        P(DP, TENSOR),
        P(DP, None),
        P(DP, None),
        P(DP, TENSOR),
        P(TENSOR, DP),
    )
    out_specs = (P(DP, TENSOR), P(DP, TENSOR), P(DP, TENSOR), P(DP, TENSOR))
    return jax.shard_map(
        per_device, mesh=torus, in_specs=in_specs, out_specs=out_specs, check_vma=False
    )
```

```python
import functools

import jax
import jax.numpy as jnp
import numpy as np
from jax import lax
from jax.experimental import pallas as pl
from jax.experimental.pallas import tpu as pltpu
from jax.sharding import Mesh
from jax.sharding import PartitionSpec as P

HD = 128
HEAD_DEV = 4
GROUP = 16
SCALE = HD ** (-0.5)
DP = ("y", "xl")
TENSOR = ("xh", "z", "c")
PIECE = 64
BLOCK = 1024
AHEAD = 3
SLOTS = AHEAD + 1
TOKENS_SEQ = 1024


def swap(x, axis):
    return lax.ppermute(x, axis, [(0, 1), (1, 0)])


def along(x, axis):
    n = lax.axis_size(axis)
    pairs = []
    for i in range(n):
        pairs.append((2 * i, 2 * ((i + 1) % n)))
        pairs.append((2 * i + 1, 2 * ((i - 1) % n) + 1))
    return lax.ppermute(x, (axis, "c"), pairs)


def gather_weight(own):
    def near_blocks(mine):
        other = swap(mine, "c")
        near = along(mine, "y")
        near_other = along(other, "y")
        return [mine, near, swap(near_other, "c")]

    blocks = near_blocks(own)
    far = along(blocks[1], "y")
    partner = swap(own, "xl")
    far_partner = swap(far, "xl")
    return blocks + [far] + near_blocks(partner) + [far_partner]


def weight_order(y, xl, step):
    moved = np.array([0, -1, 1, 2] * 2, np.int32)
    flipped = np.repeat(np.array([0, 1], np.int32), 4)
    return (y + step * moved + 4) % 4 * 2 + (xl + flipped) % 2


def gather_rows(own):
    def ring(mine):
        other = swap(mine, "c")
        near = along(mine, "z")
        near_other = along(other, "z")
        far = along(near, "z")
        return [
            mine,
            other,
            near,
            near_other,
            swap(near, "c"),
            swap(near_other, "c"),
            far,
            swap(far, "c"),
        ]

    partner = swap(own, "xh")
    return ring(own) + ring(partner)


def row_order(xh, z, c, step):
    moved = np.array([0, 0, -1, -1, 1, 1, 2, 2] * 2, np.int32)
    core = np.array([0, 1, 0, 1, 1, 0, 0, 1] * 2, np.int32)
    flipped = np.repeat(np.array([0, 1], np.int32), 8)
    return (xh + flipped) % 2 * 8 + (z + step * moved + 4) % 4 * 2 + (c + core) % 2


def wait_whole(ref, sem):
    pltpu.make_async_copy(ref, ref, sem).wait()


def fetch_rows(pieces, block, rows, sem):
    start = pl.multiple_of(block * BLOCK, BLOCK)
    for at, piece in enumerate(pieces):
        pltpu.make_async_copy(
            piece.at[:, pl.ds(start, BLOCK)], rows.at[pl.ds(at * PIECE, PIECE), :], sem
        ).start()


def terms_kernel(order, dest, *refs, side):
    count = len(side)
    pieces = refs[:16]
    attended = refs[16:18]
    outs = refs[18 : 18 + count]
    rows, right, made, right_sem, rows_sem, out_sem = refs[18 + count :]
    for which in sorted(set(side)):
        for at in range(16):
            start = pl.multiple_of(order[at] * PIECE, PIECE)
            pltpu.make_async_copy(
                attended[which].at[pl.ds(start, PIECE), :],
                right.at[which, pl.ds(at * PIECE, PIECE), :],
                right_sem.at[which],
            ).start()

    def fetch(at):
        fetch_rows(pieces, dest[at], rows.at[at % SLOTS], rows_sem.at[at % SLOTS])

    for at in range(min(2, count)):
        fetch(at)
    for which in sorted(set(side)):
        wait_whole(right.at[which], right_sem.at[which])
    for at in range(count):
        wait_whole(rows.at[at % SLOTS], rows_sem.at[at % SLOTS])
        if at + 2 < count:
            fetch(at + 2)
        made[at] = lax.dot_general(
            rows[at % SLOTS],
            right[side[at]],
            (((0,), (0,)), ((), ())),
            preferred_element_type=jnp.float32,
        ).astype(jnp.bfloat16)
        pltpu.make_async_copy(made.at[at], outs[at], out_sem.at[at]).start()
    for at in range(count):
        pltpu.make_async_copy(made.at[at], outs[at], out_sem.at[at]).wait()


def terms(order, dest, side, pieces, attended, attended_other):
    count = len(side)
    cols = attended.shape[1]
    small = pl.BlockSpec(memory_space=pltpu.SMEM)
    large = pl.BlockSpec(memory_space=pl.ANY)
    return pl.pallas_call(
        functools.partial(terms_kernel, side=side),
        in_specs=[small] * 2 + [large] * 18,
        out_specs=[large] * count,
        scratch_shapes=[
            pltpu.VMEM((SLOTS, TOKENS_SEQ, BLOCK), jnp.bfloat16),
            pltpu.VMEM((2, TOKENS_SEQ, cols), jnp.bfloat16),
            pltpu.VMEM((count, BLOCK, cols), jnp.bfloat16),
            pltpu.SemaphoreType.DMA((2,)),
            pltpu.SemaphoreType.DMA((SLOTS,)),
            pltpu.SemaphoreType.DMA((count,)),
        ],
        out_shape=[jax.ShapeDtypeStruct((BLOCK, cols), jnp.bfloat16)] * count,
        cost_estimate=pl.CostEstimate(
            flops=2 * count * BLOCK * cols * TOKENS_SEQ,
            bytes_accessed=count * 3 * 2**20,
            transcendentals=0,
        ),
    )(order, dest, *pieces, attended, attended_other)


def dot_kernel(order, place, *refs, jobs, pieces, weights, carried, final):
    count = len(carried)
    piece_refs = refs[:pieces]
    weight_refs = refs[pieces : pieces + weights]
    carried_refs = refs[pieces + weights : pieces + weights + count]
    out, rows, right, total, made, rows_sem, right_sem, carried_sem, out_sem = refs[
        pieces + weights + count :
    ]

    def rows_of(slot, first):
        return rows.at[slot, pl.ds(first * PIECE, (pieces - first) * PIECE), :]

    def fetch(at):
        slot = at % SLOTS
        block, first = jobs[at]
        fetch_rows(
            piece_refs[first:], place[block], rows_of(slot, first), rows_sem.at[slot]
        )
        pltpu.make_async_copy(weight_refs[block], right.at[slot], right_sem.at[slot]).start()

    for at in range(AHEAD):
        fetch(at)
    known = 0
    copies = []
    for at, length in enumerate(carried):
        copies.append(
            pltpu.make_async_copy(
                carried_refs[at], total.at[pl.ds(known, length), :], carried_sem.at[at]
            )
        )
        copies[-1].start()
        known += length
    if known < pieces * PIECE:
        total[known:, :] = jnp.zeros_like(total[known:, :])
    for copy in copies:
        copy.wait()
    for at, (block, first) in enumerate(jobs):
        slot = at % SLOTS
        wait_whole(rows_of(slot, first), rows_sem.at[slot])
        wait_whole(right.at[slot], right_sem.at[slot])
        if at + AHEAD < len(jobs):
            fetch(at + AHEAD)
        total[first * PIECE :, :] += jnp.dot(
            rows[slot, first * PIECE : pieces * PIECE, :],
            right[slot],
            preferred_element_type=jnp.float32,
        )
    if final:
        made[...] = total[...].astype(jnp.bfloat16)
        for at in range(pieces):
            start = pl.multiple_of(order[at] * PIECE, PIECE)
            pltpu.make_async_copy(
                made.at[pl.ds(at * PIECE, PIECE), :], out.at[pl.ds(start, PIECE), :], out_sem
            ).start()
        wait_whole(made, out_sem)
    else:
        copy = pltpu.make_async_copy(total, out, out_sem)
        copy.start()
        copy.wait()


def partial_dot(order, place, pieces, weights, jobs, carried=(), final=False):
    cols = weights[0].shape[1]
    length = len(pieces) * PIECE
    small = pl.BlockSpec(memory_space=pltpu.SMEM)
    large = pl.BlockSpec(memory_space=pl.ANY)
    kernel = functools.partial(
        dot_kernel,
        jobs=jobs,
        pieces=len(pieces),
        weights=len(weights),
        carried=tuple(x.shape[0] for x in carried),
        final=final,
    )
    flops = sum(2 * (len(pieces) - first) * PIECE * BLOCK * cols for _, first in jobs)
    return pl.pallas_call(
        kernel,
        in_specs=[small] * 2 + [large] * (len(pieces) + len(weights) + len(carried)),
        out_specs=large,
        scratch_shapes=[
            pltpu.VMEM((SLOTS, length, BLOCK), jnp.bfloat16),
            pltpu.VMEM((SLOTS, BLOCK, cols), jnp.bfloat16),
            pltpu.VMEM((length, cols), jnp.float32),
            pltpu.VMEM((length if final else PIECE, cols), jnp.bfloat16),
            pltpu.SemaphoreType.DMA((SLOTS,)),
            pltpu.SemaphoreType.DMA((SLOTS,)),
            pltpu.SemaphoreType.DMA((max(len(carried), 1),)),
            pltpu.SemaphoreType.DMA(()),
        ],
        out_shape=jax.ShapeDtypeStruct((length, cols), jnp.bfloat16 if final else jnp.float32),
        cost_estimate=pl.CostEstimate(
            flops=flops, bytes_accessed=len(jobs) * 3 * 2**20, transcendentals=0
        ),
    )(order, place, *pieces, *weights, *carried)


def grad_attention_rows(order, place, pieces, weights):
    early = tuple((block, 0) for block in range(4))
    first = partial_dot(order, place, pieces[:8], weights[:4], early)
    second = partial_dot(order, place, pieces[8:14], weights[:4], early)
    late = tuple((block, 14) for block in range(4)) + tuple((block, 0) for block in range(4, 8))
    return partial_dot(order, place, pieces, weights, late, (first, second), final=True)


QB = 256
QUARTER = HD // 4


def head_kernel(where, *refs, first, count):
    query, key, value, grad, attended, stats = refs[:6]
    step = pl.program_id(0)
    head = step + first
    if first:
        key_start, value_start, _, query_grad, kept, sent, key_part, value_part, sums = refs[6:]
    else:
        query_grad, key_part, value_part = refs[6:]

    @pl.when(step == 0)
    def _():
        key_part[...] = key_start[...] if first else jnp.zeros_like(key_part)
        value_part[...] = value_start[...] if first else jnp.zeros_like(value_part)

    for block in range(TOKENS_SEQ // QB):
        at = slice(block * QB, (block + 1) * QB)
        seen = (block + 1) * QB
        q = query[at, :]
        g = grad[at, :]
        k = key[:seen, :]
        v = value[:seen, :]
        contract = (((1,), (1,)), ((), ()))
        scores = lax.dot_general(k, q, contract, preferred_element_type=jnp.float32) * SCALE
        attention = jnp.exp(scores - stats[pl.ds(head, 1), at])
        rows = lax.broadcasted_iota(jnp.int32, (QB, QB), 0)
        cols = lax.broadcasted_iota(jnp.int32, (QB, QB), 1)
        last = jnp.where(rows <= cols, attention[seen - QB :], 0.0)
        attention = jnp.concatenate([attention[: seen - QB], last], axis=0) if block else last
        grad_attention = lax.dot_general(v, g, contract, preferred_element_type=jnp.float32)
        offset = g.astype(jnp.float32) * attended[at, :].astype(jnp.float32)
        offset = jnp.sum(offset.T, axis=0, keepdims=True)
        grad_scores = attention * (grad_attention - offset)
        grad_scores = grad_scores.astype(jnp.bfloat16)
        low = attention.astype(jnp.bfloat16)
        value_part[:seen, :] += jnp.dot(low, g, preferred_element_type=jnp.float32)
        key_part[:seen, :] += SCALE * jnp.dot(grad_scores, q, preferred_element_type=jnp.float32)
        back = lax.dot_general(
            grad_scores, k, (((0,), (0,)), ((), ())), preferred_element_type=jnp.float32
        )
        query_grad[at, :] = (back * SCALE).astype(jnp.bfloat16)

    if first:

        @pl.when(step == count - 1)
        def _():
            sums[:HD, :] = key_part[...].T
            sums[HD:, :] = value_part[...].T
            for at in range(2 * HD // (2 * QUARTER)):
                rows = slice(at * QUARTER, (at + 1) * QUARTER)
                mine = pl.multiple_of((2 * at + where[1]) * QUARTER, QUARTER)
                other = pl.multiple_of((2 * at + 1 - where[1]) * QUARTER, QUARTER)
                kept[rows, :] = sums[pl.ds(mine, QUARTER), :]
                sent[rows, :] = sums[pl.ds(other, QUARTER), :].astype(jnp.bfloat16)


def attention_grads(head_at, query, keys, values, grad_att, attended, stats):
    length = query.shape[0]
    count = HEAD_DEV // 2
    part = jax.ShapeDtypeStruct((length, HD), jnp.float32)
    scratch = [pltpu.VMEM((length, HD), jnp.float32)] * 2
    scratch += [pltpu.VMEM((2 * HD, length), jnp.float32)]
    whole = pl.BlockSpec((length, HD), lambda h, at: (0, 0))

    def call(first, more):
        column = pl.BlockSpec((length, HD), lambda h, at: (0, h + first))
        shared = pl.BlockSpec((length, HD), lambda h, at: (0, at[0]))
        row = pl.BlockSpec((HEAD_DEV, length), lambda h, at: (0, 0))
        made = [jax.ShapeDtypeStruct(query.shape, jnp.bfloat16)]
        if first:
            made_specs = [column] + [pl.BlockSpec((HD, length), lambda h, at: (0, 0))] * 2
            made += [jax.ShapeDtypeStruct((HD, length), jnp.float32)]
            made += [jax.ShapeDtypeStruct((HD, length), jnp.bfloat16)]
        else:
            made_specs = [column, whole, whole]
            made += [part, part]
        return pl.pallas_call(
            functools.partial(head_kernel, first=first, count=count),
            grid_spec=pltpu.PrefetchScalarGridSpec(
                num_scalar_prefetch=1,
                grid=(count,),
                in_specs=[column, shared, shared, column, column, row]
                + ([whole, whole, pl.BlockSpec(memory_space=pl.ANY)] if first else []),
                out_specs=made_specs,
                scratch_shapes=scratch if first else [],
            ),
            out_shape=made,
            input_output_aliases={9: 0} if first else {},
            cost_estimate=pl.CostEstimate(
                flops=10 * count * length * length * HD,
                bytes_accessed=4 * 2**20,
                transcendentals=count * length * length,
            ),
        )(head_at, query, keys, values, grad_att, attended, stats, *more)

    query_grad, key_part, value_part = call(0, ())
    return call(count, (key_part, value_part, query_grad))


def added(*parts):
    total = parts[0].astype(jnp.float32)
    for part in parts[1:]:
        total = total + part.astype(jnp.float32)
    return total.astype(jnp.bfloat16)


def weight_sums(order, pieces, attended, y, xl, step):
    attended_other = swap(attended, "c")

    def dests(moved, core, flipped):
        moved = np.array(moved, np.int32) + step * np.array(core, np.int32) + 4
        return (y + moved) % 4 * 2 + (xl + np.array(flipped, np.int32)) % 2

    def call(dest, side):
        return terms(order, dest, side, pieces, attended, attended_other)

    other_p, far_p = call(dests([0, 2], [1, 0], [1, 1]), [1, 0])
    near_p, other_o = call(dests([0, 0], [1, 1], [1, 0]), [0, 1])
    far_o, near_o, own_p, own_o = call(
        dests([2, 0, 0, 0], [0, 1, 0, 0], [0, 0, 1, 0]), [0, 0, 0, 0]
    )
    far = added(far_o, swap(far_p, "xl"))
    far = along(far, "y")
    near_p = along(near_p, "y")
    near_o = along(added(near_o, far), "y")
    other_p = swap(along(other_p, "y"), "c")
    other_o = swap(along(other_o, "y"), "c")
    partner = swap(added(own_p, near_p, other_p), "xl")
    known = own_o.astype(jnp.float32) + other_o.astype(jnp.float32)
    known = known + partner.astype(jnp.float32)
    known = lax.optimization_barrier(known)
    return added(known, near_o)


def per_device(grad_out, out_weight, query, keys, values, attended, stats):
    y, xl, xh, z, c = (lax.axis_index(name) for name in ("y", "xl", "xh", "z", "c"))
    step = 1 - 2 * c
    pieces = gather_rows(grad_out)
    weights = gather_weight(out_weight)
    order = row_order(xh, z, c, step)
    weight_grad = weight_sums(order, pieces, attended, y, xl, step)
    grad_att = grad_attention_rows(order, weight_order(y, xl, step), pieces, weights)
    key_head = (xh * 8 + z * 2 + c) * HEAD_DEV // GROUP
    query_grad, kept, sent = attention_grads(
        jnp.stack([key_head, c]), query, keys, values, grad_att, attended, stats
    )
    got = swap(sent, "c")
    parts = (kept + got.astype(jnp.float32)).reshape(2, 2, QUARTER, query.shape[0])
    mine = lax.dynamic_index_in_dim(parts, z % 2, 1, keepdims=False)
    sent = lax.dynamic_index_in_dim(parts, 1 - z % 2, 1, keepdims=False)
    pairs = [(0, 1), (1, 0), (2, 3), (3, 2)]
    got = lax.ppermute(sent.astype(jnp.bfloat16), "z", pairs)
    parts = mine + got.astype(jnp.float32)
    key_grad = parts[0].T.astype(jnp.bfloat16)
    value_grad = parts[1].T.astype(jnp.bfloat16)
    return (query_grad, key_grad, value_grad, weight_grad)


def solution(mesh):
    torus = Mesh(mesh.devices.reshape(4, 2, 2, 4, 2), DP + TENSOR)
    in_specs = (
        P(DP + TENSOR, None),
        P(DP, TENSOR),
        P(DP, TENSOR),
        P(DP, None),
        P(DP, None),
        P(DP, TENSOR),
        P(TENSOR, DP),
    )
    out_specs = (P(DP, TENSOR), P(DP, TENSOR), P(DP, TENSOR), P(DP, TENSOR))
    return jax.shard_map(
        per_device, mesh=torus, in_specs=in_specs, out_specs=out_specs, check_vma=False
    )
```

```python
import functools

import jax
import jax.numpy as jnp
import numpy as np
from jax import lax
from jax.experimental import pallas as pl
from jax.experimental.pallas import tpu as pltpu
from jax.sharding import Mesh
from jax.sharding import PartitionSpec as P

HD = 128
HEAD_DEV = 4
GROUP = 16
SCALE = HD ** (-0.5)
DP = ("y", "xl")
TENSOR = ("xh", "z", "c")
PIECE = 64
BLOCK = 1024
AHEAD = 3
SLOTS = AHEAD + 1
TOKENS_SEQ = 1024


def swap(x, axis):
    return lax.ppermute(x, axis, [(0, 1), (1, 0)])


def along(x, axis):
    n = lax.axis_size(axis)
    pairs = []
    for i in range(n):
        pairs.append((2 * i, 2 * ((i + 1) % n)))
        pairs.append((2 * i + 1, 2 * ((i - 1) % n) + 1))
    return lax.ppermute(x, (axis, "c"), pairs)


def gather_weight(own):
    def near_blocks(mine):
        other = swap(mine, "c")
        near = along(mine, "y")
        near_other = along(other, "y")
        return [mine, near, swap(near_other, "c")]

    blocks = near_blocks(own)
    far = along(blocks[1], "y")
    partner = swap(own, "xl")
    far_partner = swap(far, "xl")
    return blocks + [far] + near_blocks(partner) + [far_partner]


def weight_order(y, xl, step):
    moved = np.array([0, -1, 1, 2] * 2, np.int32)
    flipped = np.repeat(np.array([0, 1], np.int32), 4)
    return (y + step * moved + 4) % 4 * 2 + (xl + flipped) % 2


def gather_rows(own):
    def ring(mine):
        other = swap(mine, "c")
        near = along(mine, "z")
        near_other = along(other, "z")
        far = along(near, "z")
        return [
            mine,
            other,
            near,
            near_other,
            swap(near, "c"),
            swap(near_other, "c"),
            far,
            swap(far, "c"),
        ]

    partner = swap(own, "xh")
    return ring(own) + ring(partner)


def row_order(xh, z, c, step):
    moved = np.array([0, 0, -1, -1, 1, 1, 2, 2] * 2, np.int32)
    core = np.array([0, 1, 0, 1, 1, 0, 0, 1] * 2, np.int32)
    flipped = np.repeat(np.array([0, 1], np.int32), 8)
    return (xh + flipped) % 2 * 8 + (z + step * moved + 4) % 4 * 2 + (c + core) % 2


def wait_whole(ref, sem):
    pltpu.make_async_copy(ref, ref, sem).wait()


def fetch_rows(pieces, block, rows, sem):
    start = pl.multiple_of(block * BLOCK, BLOCK)
    for at, piece in enumerate(pieces):
        pltpu.make_async_copy(
            piece.at[:, pl.ds(start, BLOCK)], rows.at[pl.ds(at * PIECE, PIECE), :], sem
        ).start()


def terms_kernel(order, dest, *refs, side):
    count = len(side)
    pieces = refs[:16]
    attended = refs[16:18]
    outs = refs[18 : 18 + count]
    rows, right, made, right_sem, rows_sem, out_sem = refs[18 + count :]
    for which in sorted(set(side)):
        for at in range(16):
            start = pl.multiple_of(order[at] * PIECE, PIECE)
            pltpu.make_async_copy(
                attended[which].at[pl.ds(start, PIECE), :],
                right.at[which, pl.ds(at * PIECE, PIECE), :],
                right_sem.at[which],
            ).start()

    def fetch(at):
        fetch_rows(pieces, dest[at], rows.at[at % SLOTS], rows_sem.at[at % SLOTS])

    for at in range(min(2, count)):
        fetch(at)
    for which in sorted(set(side)):
        wait_whole(right.at[which], right_sem.at[which])
    for at in range(count):
        wait_whole(rows.at[at % SLOTS], rows_sem.at[at % SLOTS])
        if at + 2 < count:
            fetch(at + 2)
        made[at] = lax.dot_general(
            rows[at % SLOTS],
            right[side[at]],
            (((0,), (0,)), ((), ())),
            preferred_element_type=jnp.float32,
        ).astype(jnp.bfloat16)
        pltpu.make_async_copy(made.at[at], outs[at], out_sem.at[at]).start()
    for at in range(count):
        pltpu.make_async_copy(made.at[at], outs[at], out_sem.at[at]).wait()


def terms(order, dest, side, pieces, attended, attended_other):
    count = len(side)
    cols = attended.shape[1]
    small = pl.BlockSpec(memory_space=pltpu.SMEM)
    large = pl.BlockSpec(memory_space=pl.ANY)
    return pl.pallas_call(
        functools.partial(terms_kernel, side=side),
        in_specs=[small] * 2 + [large] * 18,
        out_specs=[large] * count,
        scratch_shapes=[
            pltpu.VMEM((SLOTS, TOKENS_SEQ, BLOCK), jnp.bfloat16),
            pltpu.VMEM((2, TOKENS_SEQ, cols), jnp.bfloat16),
            pltpu.VMEM((count, BLOCK, cols), jnp.bfloat16),
            pltpu.SemaphoreType.DMA((2,)),
            pltpu.SemaphoreType.DMA((SLOTS,)),
            pltpu.SemaphoreType.DMA((count,)),
        ],
        out_shape=[jax.ShapeDtypeStruct((BLOCK, cols), jnp.bfloat16)] * count,
        cost_estimate=pl.CostEstimate(
            flops=2 * count * BLOCK * cols * TOKENS_SEQ,
            bytes_accessed=count * 3 * 2**20,
            transcendentals=0,
        ),
    )(order, dest, *pieces, attended, attended_other)


def dot_kernel(order, place, *refs, jobs, pieces, weights, carried, final):
    count = len(carried)
    piece_refs = refs[:pieces]
    weight_refs = refs[pieces : pieces + weights]
    carried_refs = refs[pieces + weights : pieces + weights + count]
    out, rows, right, total, made, rows_sem, right_sem, carried_sem, out_sem = refs[
        pieces + weights + count :
    ]

    def rows_of(slot, first):
        return rows.at[slot, pl.ds(first * PIECE, (pieces - first) * PIECE), :]

    def fetch(at):
        slot = at % SLOTS
        block, first = jobs[at]
        fetch_rows(
            piece_refs[first:], place[block], rows_of(slot, first), rows_sem.at[slot]
        )
        pltpu.make_async_copy(weight_refs[block], right.at[slot], right_sem.at[slot]).start()

    for at in range(AHEAD):
        fetch(at)
    known = 0
    copies = []
    for at, length in enumerate(carried):
        copies.append(
            pltpu.make_async_copy(
                carried_refs[at], total.at[pl.ds(known, length), :], carried_sem.at[at]
            )
        )
        copies[-1].start()
        known += length
    if known < pieces * PIECE:
        total[known:, :] = jnp.zeros_like(total[known:, :])
    for copy in copies:
        copy.wait()
    for at, (block, first) in enumerate(jobs):
        slot = at % SLOTS
        wait_whole(rows_of(slot, first), rows_sem.at[slot])
        wait_whole(right.at[slot], right_sem.at[slot])
        if at + AHEAD < len(jobs):
            fetch(at + AHEAD)
        total[first * PIECE :, :] += jnp.dot(
            rows[slot, first * PIECE : pieces * PIECE, :],
            right[slot],
            preferred_element_type=jnp.float32,
        )
    if final:
        made[...] = total[...].astype(jnp.bfloat16)
        for at in range(pieces):
            start = pl.multiple_of(order[at] * PIECE, PIECE)
            pltpu.make_async_copy(
                made.at[pl.ds(at * PIECE, PIECE), :], out.at[pl.ds(start, PIECE), :], out_sem
            ).start()
        wait_whole(made, out_sem)
    else:
        copy = pltpu.make_async_copy(total, out, out_sem)
        copy.start()
        copy.wait()


def partial_dot(order, place, pieces, weights, jobs, carried=(), final=False):
    cols = weights[0].shape[1]
    length = len(pieces) * PIECE
    small = pl.BlockSpec(memory_space=pltpu.SMEM)
    large = pl.BlockSpec(memory_space=pl.ANY)
    kernel = functools.partial(
        dot_kernel,
        jobs=jobs,
        pieces=len(pieces),
        weights=len(weights),
        carried=tuple(x.shape[0] for x in carried),
        final=final,
    )
    flops = sum(2 * (len(pieces) - first) * PIECE * BLOCK * cols for _, first in jobs)
    return pl.pallas_call(
        kernel,
        in_specs=[small] * 2 + [large] * (len(pieces) + len(weights) + len(carried)),
        out_specs=large,
        scratch_shapes=[
            pltpu.VMEM((SLOTS, length, BLOCK), jnp.bfloat16),
            pltpu.VMEM((SLOTS, BLOCK, cols), jnp.bfloat16),
            pltpu.VMEM((length, cols), jnp.float32),
            pltpu.VMEM((length if final else PIECE, cols), jnp.bfloat16),
            pltpu.SemaphoreType.DMA((SLOTS,)),
            pltpu.SemaphoreType.DMA((SLOTS,)),
            pltpu.SemaphoreType.DMA((max(len(carried), 1),)),
            pltpu.SemaphoreType.DMA(()),
        ],
        out_shape=jax.ShapeDtypeStruct((length, cols), jnp.bfloat16 if final else jnp.float32),
        cost_estimate=pl.CostEstimate(
            flops=flops, bytes_accessed=len(jobs) * 3 * 2**20, transcendentals=0
        ),
    )(order, place, *pieces, *weights, *carried)


def grad_attention_rows(order, place, pieces, weights):
    early = tuple((block, 0) for block in range(4))
    first = partial_dot(order, place, pieces[:8], weights[:4], early)
    second = partial_dot(order, place, pieces[8:14], weights[:4], early)
    late = tuple((block, 14) for block in range(4)) + tuple((block, 0) for block in range(4, 8))
    return partial_dot(order, place, pieces, weights, late, (first, second), final=True)


QB = 256
QUARTER = HD // 4


def head_kernel(where, *refs, first, count):
    query, key, value, grad, attended, stats = refs[:6]
    step = pl.program_id(0)
    head = step + first
    if first:
        key_start, value_start, _, query_grad, kept, sent, key_part, value_part, sums = refs[6:]
    else:
        query_grad, key_part, value_part = refs[6:]

    @pl.when(step == 0)
    def _():
        key_part[...] = key_start[...] if first else jnp.zeros_like(key_part)
        value_part[...] = value_start[...] if first else jnp.zeros_like(value_part)

    for block in range(TOKENS_SEQ // QB):
        at = slice(block * QB, (block + 1) * QB)
        seen = (block + 1) * QB
        q = query[at, :]
        g = grad[at, :]
        k = key[:seen, :]
        v = value[:seen, :]
        contract = (((1,), (1,)), ((), ()))
        scores = lax.dot_general(k, q, contract, preferred_element_type=jnp.float32) * SCALE
        attention = jnp.exp(scores - stats[pl.ds(head, 1), at])
        rows = lax.broadcasted_iota(jnp.int32, (QB, QB), 0)
        cols = lax.broadcasted_iota(jnp.int32, (QB, QB), 1)
        last = jnp.where(rows <= cols, attention[seen - QB :], 0.0)
        attention = jnp.concatenate([attention[: seen - QB], last], axis=0) if block else last
        grad_attention = lax.dot_general(v, g, contract, preferred_element_type=jnp.float32)
        offset = g.astype(jnp.float32) * attended[at, :].astype(jnp.float32)
        offset = jnp.sum(offset.T, axis=0, keepdims=True)
        grad_scores = attention * (grad_attention - offset)
        grad_scores = grad_scores.astype(jnp.bfloat16)
        low = attention.astype(jnp.bfloat16)
        value_part[:seen, :] += jnp.dot(low, g, preferred_element_type=jnp.float32)
        key_part[:seen, :] += SCALE * jnp.dot(grad_scores, q, preferred_element_type=jnp.float32)
        back = lax.dot_general(
            grad_scores, k, (((0,), (0,)), ((), ())), preferred_element_type=jnp.float32
        )
        query_grad[at, :] = (back * SCALE).astype(jnp.bfloat16)

    if first:

        @pl.when(step == count - 1)
        def _():
            sums[:HD, :] = key_part[...].T
            sums[HD:, :] = value_part[...].T
            for at in range(2 * HD // (2 * QUARTER)):
                rows = slice(at * QUARTER, (at + 1) * QUARTER)
                mine = pl.multiple_of((2 * at + where[1]) * QUARTER, QUARTER)
                other = pl.multiple_of((2 * at + 1 - where[1]) * QUARTER, QUARTER)
                kept[rows, :] = sums[pl.ds(mine, QUARTER), :]
                sent[rows, :] = sums[pl.ds(other, QUARTER), :].astype(jnp.bfloat16)


def attention_grads(head_at, query, keys, values, grad_att, attended, stats):
    length = query.shape[0]
    count = HEAD_DEV // 2
    part = jax.ShapeDtypeStruct((length, HD), jnp.float32)
    scratch = [pltpu.VMEM((length, HD), jnp.float32)] * 2
    scratch += [pltpu.VMEM((2 * HD, length), jnp.float32)]
    whole = pl.BlockSpec((length, HD), lambda h, at: (0, 0))

    def call(first, more):
        column = pl.BlockSpec((length, HD), lambda h, at: (0, h + first))
        shared = pl.BlockSpec((length, HD), lambda h, at: (0, at[0]))
        row = pl.BlockSpec((HEAD_DEV, length), lambda h, at: (0, 0))
        made = [jax.ShapeDtypeStruct(query.shape, jnp.bfloat16)]
        if first:
            made_specs = [column] + [pl.BlockSpec((HD, length), lambda h, at: (0, 0))] * 2
            made += [jax.ShapeDtypeStruct((HD, length), jnp.float32)]
            made += [jax.ShapeDtypeStruct((HD, length), jnp.bfloat16)]
        else:
            made_specs = [column, whole, whole]
            made += [part, part]
        return pl.pallas_call(
            functools.partial(head_kernel, first=first, count=count),
            grid_spec=pltpu.PrefetchScalarGridSpec(
                num_scalar_prefetch=1,
                grid=(count,),
                in_specs=[column, shared, shared, column, column, row]
                + ([whole, whole, pl.BlockSpec(memory_space=pl.ANY)] if first else []),
                out_specs=made_specs,
                scratch_shapes=scratch if first else [],
            ),
            out_shape=made,
            input_output_aliases={9: 0} if first else {},
            cost_estimate=pl.CostEstimate(
                flops=10 * count * length * length * HD,
                bytes_accessed=4 * 2**20,
                transcendentals=count * length * length,
            ),
        )(head_at, query, keys, values, grad_att, attended, stats, *more)

    query_grad, key_part, value_part = call(0, ())
    return call(count, (key_part, value_part, query_grad))


def added(*parts):
    total = parts[0].astype(jnp.float32)
    for part in parts[1:]:
        total = total + part.astype(jnp.float32)
    return total.astype(jnp.bfloat16)


def weight_sums(order, pieces, attended, y, xl, step):
    attended_other = swap(attended, "c")

    def dests(moved, core, flipped):
        moved = np.array(moved, np.int32) + step * np.array(core, np.int32) + 4
        return (y + moved) % 4 * 2 + (xl + np.array(flipped, np.int32)) % 2

    def call(dest, side):
        return terms(order, dest, side, pieces, attended, attended_other)

    other_p, far_p = call(dests([0, 2], [1, 0], [1, 1]), [1, 0])
    near_p, other_o, far_o = call(dests([0, 0, 2], [1, 1, 0], [1, 0, 0]), [0, 1, 0])
    near_o, own_p, own_o = call(dests([0, 0, 0], [1, 0, 0], [0, 1, 0]), [0, 0, 0])
    far = added(far_o, swap(far_p, "xl"))
    far = along(far, "y")
    near_p = along(near_p, "y")
    near_o = along(added(near_o, far), "y")
    other_p = swap(along(other_p, "y"), "c")
    other_o = swap(along(other_o, "y"), "c")
    partner = swap(added(own_p, near_p, other_p), "xl")
    known = own_o.astype(jnp.float32) + other_o.astype(jnp.float32)
    known = known + partner.astype(jnp.float32)
    known = lax.optimization_barrier(known)
    return added(known, near_o)


def per_device(grad_out, out_weight, query, keys, values, attended, stats):
    y, xl, xh, z, c = (lax.axis_index(name) for name in ("y", "xl", "xh", "z", "c"))
    step = 1 - 2 * c
    pieces = gather_rows(grad_out)
    weights = gather_weight(out_weight)
    order = row_order(xh, z, c, step)
    weight_grad = weight_sums(order, pieces, attended, y, xl, step)
    grad_att = grad_attention_rows(order, weight_order(y, xl, step), pieces, weights)
    key_head = (xh * 8 + z * 2 + c) * HEAD_DEV // GROUP
    query_grad, kept, sent = attention_grads(
        jnp.stack([key_head, c]), query, keys, values, grad_att, attended, stats
    )
    got = swap(sent, "c")
    parts = (kept + got.astype(jnp.float32)).reshape(2, 2, QUARTER, query.shape[0])
    mine = lax.dynamic_index_in_dim(parts, z % 2, 1, keepdims=False)
    sent = lax.dynamic_index_in_dim(parts, 1 - z % 2, 1, keepdims=False)
    pairs = [(0, 1), (1, 0), (2, 3), (3, 2)]
    got = lax.ppermute(sent.astype(jnp.bfloat16), "z", pairs)
    parts = mine + got.astype(jnp.float32)
    key_grad = parts[0].T.astype(jnp.bfloat16)
    value_grad = parts[1].T.astype(jnp.bfloat16)
    return (query_grad, key_grad, value_grad, weight_grad)


def solution(mesh):
    torus = Mesh(mesh.devices.reshape(4, 2, 2, 4, 2), DP + TENSOR)
    in_specs = (
        P(DP + TENSOR, None),
        P(DP, TENSOR),
        P(DP, TENSOR),
        P(DP, None),
        P(DP, None),
        P(DP, TENSOR),
        P(TENSOR, DP),
    )
    out_specs = (P(DP, TENSOR), P(DP, TENSOR), P(DP, TENSOR), P(DP, TENSOR))
    return jax.shard_map(
        per_device, mesh=torus, in_specs=in_specs, out_specs=out_specs, check_vma=False
    )
```
